32 devices in a mesh: gx: 2 (over x), gy: 4 (over z), gz: 4 (over y, core).
Axes of the slice: x: 2, y: 2, z: 4, core: 2. Of those that a mesh axis runs over, the one named last changes fastest.
Arguments:
- tokens: bfloat16 [512, 49, 512], P(('gx', 'gy', 'gz')), may hold values from -6 to 6
- cotangent: bfloat16 [512, 49, 512], P(('gx', 'gy', 'gz')), may hold values from -6 to 6
- regions: int32 [512, 49], P(('gx', 'gy', 'gz')), may hold values from 0 to 3
- rel_index: int32 [49, 49], replicated, may hold values from 0 to 168
- w_qkv: bfloat16 [512, 1536], replicated, may hold values from -0.25 to 0.25
- w_proj: bfloat16 [512, 512], replicated, may hold values from -0.25 to 0.25
- bias_table: float32 [169, 16], replicated, may hold values from -4 to 4
- mom_qkv: float32 [786432], P(('gx', 'gy', 'gz')), may hold values from -0.06 to 0.06
- mom_proj: float32 [262144], P(('gx', 'gy', 'gz')), may hold values from -0.06 to 0.06
- mom_table: float32 [169, 16], replicated, may hold values from -0.06 to 0.06
Outputs:
- new_mom_qkv: float32 [786432], P(('gx', 'gy', 'gz'))
- new_mom_proj: float32 [262144], P(('gx', 'gy', 'gz'))
- new_mom_table: float32 [169, 16], replicated
The draws below stay inside these ranges and needn't reach their ends.
All inputs are finite; a program needn't handle non-finite values.
Results may differ from the reference program's by a relative error of at most 0.015.
Values sent between devices are 32-bit elements; how exact they have to be, the bound alone decides.
A program may use at most 128 MiB of HBM per device.

```python
import jax
import jax.numpy as jnp
from jax import lax

D = 512
HEADS = 16
WIN_TOK = 49
TABLE = 169
WIN_DEV = 16
WINDOWS = 512
N_GX = 2
N_GY = 4
N_GZ = 4


def touch_ends(drawn, own_key, smallest, largest):
    dims = drawn.shape
    index_at = [jax.random.randint(jax.random.fold_in(own_key, axis), (), 0, dims[axis]) for axis in range(len(dims))]
    drawn = drawn.at[tuple(index_at)].set(smallest)
    longest = dims.index(max(dims))
    index_at[longest] = (index_at[longest] + 1) % dims[longest]
    return drawn.at[tuple(index_at)].set(largest)


def block_levels(key, shape, cuts, low, largest):
    def one(dim, shards_of):
        steps = jax.random.uniform(jax.random.fold_in(jax.random.fold_in(key, 6), dim), (shards_of,), jnp.float32, low / len(cuts), largest / len(cuts))
        return jnp.repeat(jnp.exp(steps), shape[dim] // shards_of).reshape((-1,) + (1,) * (len(shape) - dim - 1))

    loudness = one(*cuts[0])
    for cut in cuts[1:]:
        loudness = loudness * one(*cut)
    return loudness


def noise(stream_key, extent, deviation, reach, cuts=(), held_as=jnp.bfloat16):
    drawn = deviation * jax.random.normal(stream_key, extent, jnp.float32)
    if cuts:
        drawn = drawn * block_levels(stream_key, extent, cuts, -0.22, 0.18)
    return jnp.clip(drawn, -reach, reach).astype(held_as)


def setup_inputs(seed: int = 0) -> dict:
    key_list = jax.random.split(jax.random.key(seed), 11)
    return {
        "tokens": noise(key_list[0], (WINDOWS, WIN_TOK, D), 1.0, 6.0, ((0, 32),)),
        "cotangent": noise(key_list[1], (WINDOWS, WIN_TOK, D), 1.0, 6.0, ((0, 32),)),
        "regions": touch_ends(jax.random.randint(key_list[2], (WINDOWS, WIN_TOK), 0, 4), jax.random.fold_in(key_list[2], 1), 0, 3).astype(jnp.int32),
        "rel_index": touch_ends(jax.random.randint(key_list[3], (WIN_TOK, WIN_TOK), 0, 169), jax.random.fold_in(key_list[3], 1), 0, 168).astype(jnp.int32),
        "w_qkv": noise(key_list[4], (D, 3 * D), D ** -0.5, 0.25),
        "w_proj": noise(key_list[5], (D, D), D ** -0.5, 0.25),
        "bias_table": noise(key_list[6], (TABLE, HEADS), 1.0, 4.0, (), jnp.float32),
        "mom_qkv": noise(key_list[7], (3 * D * D,), 0.01, 0.06, ((0, 32),), jnp.float32),
        "mom_proj": noise(key_list[8], (D * D,), 0.01, 0.06, ((0, 32),), jnp.float32),
        "mom_table": noise(key_list[9], (TABLE, HEADS), 0.01, 0.06, (), jnp.float32),
    }


def attend_core(qkv, table, regions, rel_index, heads):
    win, count, width = qkv.shape
    dim = width // 3
    parts = qkv.reshape(win, count, 3, heads, dim // heads).astype(jnp.float32)
    bias = jnp.transpose(table[rel_index], (2, 0, 1))
    scores = jnp.einsum('wihc,wjhc->whij', parts[:, :, 0], parts[:, :, 1]) * (dim // heads) ** (-0.5)
    masked = jnp.where(regions[:, :, None] == regions[:, None, :], 0.0, -100.0).astype(jnp.float32)
    scores = scores + bias[None] + masked[:, None]
    probs = jax.nn.softmax(scores, axis=-1).astype(jnp.bfloat16)
    attended = jnp.einsum('whij,wjhc->wihc', probs.astype(jnp.float32), parts[:, :, 2])
    return attended.astype(jnp.bfloat16).reshape(win, count, dim)

def local_grads(tokens, cotangent, regions, rel_index, w_qkv, w_proj, bias_table, heads):
    win, count, dim = tokens.shape
    flat = tokens.reshape(win * count, dim)
    qkv = jnp.dot(flat, w_qkv, preferred_element_type=jnp.float32).astype(jnp.bfloat16).reshape(win, count, 3 * dim)

    def forward(values, table):
        return attend_core(values, table, regions, rel_index, heads)
    attended, pullback = jax.vjp(forward, qkv, bias_table)
    flat_dy = cotangent.reshape(win * count, dim)
    grad_proj = jnp.dot(attended.reshape(win * count, dim).astype(jnp.float32).T, flat_dy.astype(jnp.float32))
    d_attended = jnp.dot(flat_dy, w_proj.T, preferred_element_type=jnp.float32).astype(jnp.bfloat16)
    d_qkv, grad_table = pullback(d_attended.reshape(win, count, dim))
    grad_qkv = jnp.dot(flat.astype(jnp.float32).T, d_qkv.reshape(win * count, 3 * dim).astype(jnp.float32))
    return (grad_qkv, grad_proj, grad_table)

def reference(tokens, cotangent, regions, rel_index, w_qkv, w_proj, bias_table, mom_qkv, mom_proj, mom_table):
    groups = N_GX * N_GY * N_GZ
    heads = bias_table.shape[1]
    tok_groups = tokens.reshape(groups, WIN_DEV, WIN_TOK, D)
    cot_groups = cotangent.reshape(groups, WIN_DEV, WIN_TOK, D)
    reg_groups = regions.reshape(groups, WIN_DEV, WIN_TOK)

    def step(carry, items):
        g_qkv, g_proj, g_table = local_grads(items[0], items[1], items[2], rel_index, w_qkv, w_proj, bias_table, heads)
        return ((carry[0] + g_qkv, carry[1] + g_proj, carry[2] + g_table), None)
    start = (jnp.zeros(w_qkv.shape, jnp.float32), jnp.zeros(w_proj.shape, jnp.float32), jnp.zeros(bias_table.shape, jnp.float32))
    sums, unused = lax.scan(step, start, (tok_groups, cot_groups, reg_groups))
    scale = 1.0 / (WIN_DEV * groups)
    return (0.9 * mom_qkv + sums[0].reshape(-1) * scale, 0.9 * mom_proj + sums[1].reshape(-1) * scale, 0.9 * mom_table + sums[2] * scale)
```

```python
import functools
import math

import jax
import jax.numpy as jnp
from jax import lax
from jax.experimental import pallas as pl
from jax.experimental.pallas import tpu as pltpu
from jax.sharding import PartitionSpec as P

AXES = ("gx", "gy", "gz")
MESH = pl.DeviceIdType.MESH
F32, BF16 = jnp.float32, jnp.bfloat16
PAD = 64
GROUP = 4
LOG2E = math.log2(math.e)
NT = (((1,), (1,)), ((), ()))
TN = (((0,), (0,)), ((), ()))
COPIES = 8
DUE = (3, 6, 5, 7)


def dot(a, b, dims=(((1,), (0,)), ((), ()))):
    return lax.dot_general(a, b, dims, preferred_element_type=F32)


def spread(value, lanes, width):
    return jnp.concatenate(
        [jnp.where(lanes // width == h, value, jnp.zeros_like(value)) for h in range(GROUP)], axis=0
    )


def gather_heads(value, lanes, width):
    total = jnp.where(lanes // width == 0, value[:PAD], 0.0)
    for h in range(1, GROUP):
        total = jnp.where(lanes // width == h, value[h * PAD : (h + 1) * PAD], total)
    return total


class Place:
    def __init__(self):
        gx, gy, gz = (lax.axis_index(a) for a in AXES)
        self.x, self.z = gx, gy
        self.core, self.y = gz % 2, gz // 2
        self.to_core = (gx, gy, gz + 1 - 2 * self.core)
        self.to_x = (1 - gx, gy, gz)
        self.to_y = (gx, gy, gz + 2 - 4 * self.y)
        self.to_xy = (1 - gx, gy, gz + 2 - 4 * self.y)
        self.others = [(gy + k) % 4 for k in range(1, 4)]
        self.to_z = [(gx, there, gz) for there in self.others]

    def everyone(self):
        return [self.to_core, self.to_x, self.to_y, self.to_xy, *self.to_z]


class Chunk:
    def __init__(self, place, refs, send, recv, due, finish):
        self.p = place
        self.buf, self.r0, self.r1, self.r2, self.s2, self.r3 = refs
        self.send, self.recv, self.finish = send, recv, finish
        self.ab = ((place.x, place.y), (place.y, place.x))
        self.via = ((place.to_x, place.to_y), (place.to_y, place.to_x))
        self.stage, self.due = 0, due

    def copy(self, n, src, dst, there):
        return pltpu.make_async_remote_copy(
            src_ref=src,
            dst_ref=dst,
            send_sem=self.send.at[n],
            recv_sem=self.recv.at[n],
            device_id=there,
            device_id_type=MESH,
        )

    def copies(self, stage):
        p, buf = self.p, self.buf
        if stage == 0:
            return [self.copy(0, buf.at[1 - p.core], self.r0, p.to_core)]
        if stage == 1:
            return [
                self.copy(1 + h, buf.at[p.core, h, 1 - self.ab[h][0]], self.r1.at[h], self.via[h][0])
                for h in range(2)
            ]
        if stage == 2:
            return [
                self.copy(
                    3 + h,
                    buf.at[p.core, h, self.ab[h][0], 1 - self.ab[h][1]],
                    self.r2.at[h],
                    self.via[h][1],
                )
                for h in range(2)
            ]
        return [self.copy(5 + k, self.s2.at[p.others[k]], self.r3.at[k], p.to_z[k]) for k in range(3)]

    def start(self):
        for c in self.copies(0):
            c.start()

    def advance(self):
        p, buf, stage = self.p, self.buf, self.stage
        waited = self.copies(stage)
        after = self.copies(stage + 1) if stage < 3 else []
        if stage == 0:
            waited[0].wait()
            for h in range(2):
                away = 1 - self.ab[h][0]
                at = (p.core, h, away)
                buf[at] = buf[at] + self.r0[h, away]
                after[h].start()
        elif stage == 1:
            for h in range(2):
                a, b = self.ab[h]
                waited[h].wait()
                at = (p.core, h, a, 1 - b)
                buf[at] = buf[at] + self.r0[h, a, 1 - b] + self.r1[h, 1 - b]
                after[h].start()
        elif stage == 2:
            for h in range(2):
                a, b = self.ab[h]
                waited[h].wait()
                self.s2[:, h] = (
                    buf[p.core, h, a, b] + self.r0[h, a, b] + self.r1[h, b] + self.r2[h]
                )
            for c in after:
                c.start()
        else:
            for c in waited:
                c.wait()
            self.finish(self.s2[p.z] + self.r3[0] + self.r3[1] + self.r3[2])
        self.stage += 1


class Table:
    def __init__(self, place, refs, send, recv, due, finish):
        self.p = place
        self.t0, self.r0, self.t1, self.r1, self.r2 = refs
        self.send, self.recv, self.finish = send, recv, finish
        self.stage, self.due = 1, due

    def copy(self, n, src, dst, there):
        return pltpu.make_async_remote_copy(
            src_ref=src,
            dst_ref=dst,
            send_sem=self.send.at[n],
            recv_sem=self.recv.at[n],
            device_id=there,
            device_id_type=MESH,
        )

    def copies(self, stage):
        p = self.p
        if stage == 1:
            return [self.copy(0, self.t0, self.r0, p.to_core)]
        if stage == 2:
            return [
                self.copy(1 + k, self.t1, self.r1.at[k], there)
                for k, there in enumerate((p.to_x, p.to_y, p.to_xy))
            ]
        return [self.copy(4 + k, self.r2.at[p.z], self.r2.at[p.z], p.to_z[k]) for k in range(3)]

    def start(self):
        for c in self.copies(1):
            c.start()

    def advance(self):
        for c in self.copies(self.stage):
            if self.stage < 3:
                c.wait()
            else:
                c.wait_send()
        if self.stage == 1:
            self.t1[...] = self.t0[...] + self.r0[...]
        elif self.stage == 2:
            self.r2[self.p.z] = (self.t1[...] + self.r1[0]) + (self.r1[1] + self.r1[2])
        else:
            for k in range(3):
                there = (self.p.z + 3 - k) % 4
                self.copy(4 + k, self.r2.at[there], self.r2.at[there], self.p.to_z[k]).wait_recv()
            self.finish((self.r2[0] + self.r2[1]) + (self.r2[2] + self.r2[3]))
        if self.stage < 3:
            for c in self.copies(self.stage + 1):
                c.start()
        self.stage += 1


def kernel(dims, names, *all_refs):
    win, count, dim, heads, entries, remote, norm = dims
    r = dict(zip(names, all_refs, strict=True))
    width = dim // heads
    groups = heads // GROUP
    wide = GROUP * width
    scale = width**-0.5
    x, xt, c, qkv, d_att, att = r["x"], r["xt"], r["c"], r["qkv"], r["d_att"], r["att"]
    d_v, d_qk, probs, masks = r["d_v"], r["d_qk"], r["probs"], r["masks"]
    bias, bias_rows, d_bias, small, rel_t, tab = (
        r[n] for n in ("bias", "bias_rows", "d_bias", "small", "rel_t", "tab")
    )
    fetched = [("tok", "tok_v"), ("w_qkv", "w_qkv_v"), ("cot", "cot_v"), ("w_proj", "w_proj_v")]
    fetch = [
        pltpu.make_async_copy(r[a], r[b], r["fetch"].at[n]) for n, (a, b) in enumerate(fetched)
    ]
    for f in fetch:
        f.start()
    w_qkv, w_proj = r["w_qkv_v"], r["w_proj_v"]

    if remote:
        place = Place()
        barrier = pltpu.get_barrier_semaphore()
        for there in place.everyone():
            pl.semaphore_signal(barrier, inc=1, device_id=there, device_id_type=MESH)

    lanes = lax.broadcasted_iota(jnp.int32, (PAD, wide), 1)

    small[...] = jnp.zeros_like(small)
    small[0:win, 0:count] = r["reg"][...].astype(F32)
    reg_rows = small[...]
    reg_cols = reg_rows.T
    for w in range(win):
        row = reg_rows[w : w + 1, :PAD]
        row = jnp.concatenate([row, row], axis=1)
        masks[w * PAD : (w + 1) * PAD, :] = jnp.where(
            reg_cols[:PAD, w : w + 1] == row, 0.0, -100.0 * LOG2E
        )

    small[...] = jnp.full_like(small, -1.0)
    small[0:count, 0:count] = r["rel"][...].astype(F32)
    rel_t[...] = small[...].T
    tab[...] = jnp.zeros_like(tab)
    tab[:, 0:entries] = r["table"][...]
    size = tab.shape[1]
    tab_t = tab[...]
    high = tab_t.astype(BF16)
    low = (tab_t - high.astype(F32)).astype(BF16)
    both = jnp.concatenate([high, low], axis=0)
    entry = lax.broadcasted_iota(jnp.int32, (size, 128), 0).astype(F32)
    unroll = next(u for u in (7, 8, 4, 2, 1) if count % u == 0)

    def one_hot(j):
        return jnp.where(entry == rel_t[pl.ds(j, 1), :], 1.0, 0.0).astype(BF16)

    bias_rows[...] = jnp.full_like(bias_rows, -1e30)

    def look(i, carry):
        for u in range(unroll):
            j = i * unroll + u
            found = dot(both, one_hot(j))
            bias_rows[pl.ds(pl.multiple_of(j * heads, heads), heads), :] = (
                found[:heads] + found[heads:]
            ) * LOG2E
        return carry

    lax.fori_loop(0, count // unroll, look, 0)
    for g in range(groups):
        bias[g] = jnp.concatenate(
            [bias_rows[pl.ds(g * GROUP + h, PAD, stride=heads), :][:, :PAD] for h in range(GROUP)],
            axis=1,
        )
    d_bias[...] = jnp.zeros_like(d_bias)

    flat = r["flat"]
    rows_all = win * PAD
    for n in range(dim // 128):
        flat[n, count * win :, :] = jnp.zeros((rows_all - count * win, 128), F32)

    def by_window(src, dst):
        for n in range(dim // 128):
            cols = slice(n * 128, n * 128 + 128)
            for t in range(count):
                flat[n, t * win : (t + 1) * win, :] = src[t, :, cols].astype(F32)
            for w in range(win):
                dst[w * PAD : (w + 1) * PAD, cols] = flat[n, pl.ds(w, PAD, stride=win), :].astype(BF16)

    fetch[0].wait()
    by_window(r["tok_v"], x)
    fetch[2].wait()
    by_window(r["cot_v"], c)
    fetch[1].wait()
    fetch[3].wait()

    @pl.loop(0, rows_all // 256)
    def _(i):
        rows = pl.ds(pl.multiple_of(i * 256, 256), 256)
        qkv[rows, :] = dot(x[rows, :], w_qkv[...]).astype(BF16)
        d_att[rows, :] = dot(c[rows, :], w_proj[...], NT).astype(BF16)

    xt[...] = x[...].T

    def rows_of(w):
        at = w * PAD
        return pl.ds(at if isinstance(at, int) else pl.multiple_of(at, PAD), PAD)

    def part(ref, which, g, rows):
        at = which * dim + g * wide
        return ref[rows, at : at + wide]

    def forward(w, carry):
        rows = rows_of(w)
        mask = masks[rows, :]
        mask = jnp.concatenate([mask] * (GROUP * PAD // 128), axis=1)
        every = range(groups)
        queries = [spread(part(qkv, 0, g, rows), lanes, width) for g in every]
        d_out = [spread(part(d_att, 0, g, rows), lanes, width) for g in every]
        scores = [dot(part(qkv, 1, g, rows), queries[g], NT) for g in every]
        scores = [scores[g] * (scale * LOG2E) + bias[g] + mask for g in every]
        raised = [jnp.exp2(v - jnp.max(v, axis=0, keepdims=True)) for v in scores]
        p = [(v * (1.0 / jnp.sum(v, axis=0, keepdims=True))).astype(BF16) for v in raised]
        mixed = [dot(p[g], part(qkv, 2, g, rows), TN) for g in every]
        d_v[rows, :] = jnp.concatenate([dot(p[g], d_out[g]) for g in every], axis=1).astype(BF16)
        joined = [gather_heads(v, lanes, width).astype(BF16) for v in mixed]
        att[rows, :] = jnp.concatenate(joined, axis=1)
        for g in every:
            probs[g, rows, :] = p[g]
        return carry

    lax.fori_loop(0, win, forward, 0)

    tick = 0
    active = []

    def put(value, ref):
        for d in range(value.shape[0] // 16):
            dx, dz, dy, dc = d // 16, (d // 4) % 4, (d // 2) % 2, d % 2
            for half in range(2):
                a, b = (dx, dy) if half == 0 else (dy, dx)
                ref[dc, half, a, b, dz] = value[16 * d + 8 * half : 16 * d + 8 * half + 8]

    def update(out, mom, at, tiles, value):
        for half in range(2):
            for n in range(value.shape[2] // 128):
                rows = pl.ds(half * 8 * tiles + at(n), 8, stride=tiles)
                out[rows, :] = 0.9 * mom[rows, :] + value[half, :, n * 128 : n * 128 + 128] * norm

    def ship(name, n, value, finish):
        refs = [r[f"{name}_{k}"] for k in ("buf", "r0", "r1", "r2", "s2", "r3")]
        put(value, refs[0])
        chunk = Chunk(place, refs, r["send"].at[n], r["recv"].at[n], tick + DUE[0], finish)
        chunk.start()
        active.append(chunk)

    def run_due(limit):
        while True:
            ready = [k for k in active if k.stage < 4 and k.due <= limit]
            if not ready:
                return
            first = min(ready, key=lambda k: k.due)
            first.advance()
            if first.stage < 4:
                first.due += DUE[first.stage]

    if remote:
        pl.semaphore_wait(barrier, len(place.everyone()))
    tiles = dim // 128
    g_v = dot(xt[...], d_v[...])
    if remote:
        ship("v", 0, g_v, functools.partial(update, r["out_qkv"], r["mom_qkv"], lambda n: 2 * tiles + n, 3 * tiles))
    else:
        r["out_qkv"][:, 2 * dim :] = g_v
    g_proj = dot(att[...], c[...], TN)
    tick += 2
    if remote:
        ship("p", 1, g_proj, functools.partial(update, r["out_proj"], r["mom_proj"], lambda n: n, tiles))
    else:
        r["out_proj"][...] = g_proj

    def backward(g, windows):
        rows = [rows_of(w) for w in windows]
        queries = [spread(part(qkv, 0, g, rw), lanes, width) for rw in rows]
        d_out = [spread(part(d_att, 0, g, rw), lanes, width) for rw in rows]
        p = [probs[g, rw, :] for rw in rows]
        every = range(len(rows))
        d_probs = [dot(part(qkv, 2, g, rows[n]), d_out[n], NT) for n in every]
        pf = [v.astype(F32) for v in p]
        weighted = [pf[n] * d_probs[n] for n in every]
        d_scores = [
            weighted[n] - pf[n] * jnp.sum(weighted[n], axis=0, keepdims=True) for n in every
        ]
        d_bias[g] += sum(d_scores[1:], d_scores[0])
        ds = [v.astype(BF16) for v in d_scores]
        d_k = [dot(ds[n], queries[n]) * scale for n in every]
        d_q = [dot(ds[n], part(qkv, 1, g, rows[n]), TN) for n in every]
        d_q = [gather_heads(v, lanes, width) * scale for v in d_q]
        for n in every:
            d_qk[rows[n], :] = jnp.concatenate([d_q[n], d_k[n]], axis=1).astype(BF16)

    pieces = 4
    for g in range(groups):
        for s in range(pieces):
            backward(g, range(s * win // pieces, (s + 1) * win // pieces))
            tick += 1
            if remote:
                run_due(tick)
        g_qk = dot(xt[...], d_qk[...])
        tick += 1
        per = wide // 128
        if remote:
            at = lambda n, g=g: (n // per) * tiles + g * per + n % per
            ship(f"k{g}", 2 + g, g_qk, functools.partial(update, r["out_qkv"], r["mom_qkv"], at, 3 * tiles))
        else:
            for which in range(2):
                at = which * dim + g * wide
                r["out_qkv"][:, at : at + wide] = g_qk[:, which * wide : (which + 1) * wide]

    for g in range(groups):
        for h in range(GROUP):
            piece = d_bias[g, :, h * PAD : (h + 1) * PAD]
            bias_rows[pl.ds(g * GROUP + h, PAD, stride=heads), :] = jnp.concatenate(
                [piece, jnp.zeros_like(piece)], axis=1
            )

    def collect(i, total):
        for u in range(unroll):
            j = i * unroll + u
            value = bias_rows[pl.ds(pl.multiple_of(j * heads, heads), heads), :]
            top = value.astype(BF16)
            rest_of = (value - top.astype(F32)).astype(BF16)
            total = total + dot(jnp.concatenate([top, rest_of], axis=0), one_hot(j), NT)
        return total

    if remote:
        tick += 1
        run_due(tick)
    g_table = lax.fori_loop(0, count // unroll, collect, jnp.zeros((2 * heads, size), F32))
    g_table = g_table[:heads] + g_table[heads:]
    if not remote:
        r["out_table"][...] = g_table[:, :entries]
        return
    tick += 2
    refs = [r[f"t_{k}"] for k in ("t0", "r0", "t1", "r1", "r2")]
    refs[0][...] = g_table

    def table_done(value):
        r["out_table"][...] = 0.9 * r["mom_table"][...] + value[:, :entries] * norm

    last = Table(place, refs, r["send"].at[2 + groups], r["recv"].at[2 + groups], tick + 2, table_done)
    last.start()
    active.append(last)
    run_due(10**6)


def local_grads(remote, norm, tokens, cotangent, regions, rel_index, w_qkv, w_proj, bias_table, moms):
    win, count, dim = tokens.shape
    entries, heads = bias_table.shape
    groups = heads // GROUP
    rows = win * PAD
    wide = GROUP * (dim // heads)
    size = -(-entries // 128) * 128
    own = dim // 32
    inputs = dict(
        tok=tokens.transpose(1, 0, 2),
        cot=cotangent.transpose(1, 0, 2),
        reg=regions,
        rel=rel_index,
        w_qkv=w_qkv,
        w_proj=w_proj,
        table=bias_table.T,
    )
    if remote:
        inputs |= dict(
            mom_qkv=moms[0].reshape(-1, 128), mom_proj=moms[1].reshape(-1, 128), mom_table=moms[2].T
        )
        outs = dict(
            out_qkv=(own * 3 * dim // 128, 128), out_proj=(own * dim // 128, 128), out_table=(heads, entries)
        )
    else:
        outs = dict(out_qkv=(dim, 3 * dim), out_proj=(dim, dim), out_table=(heads, entries))
    vmem = pltpu.VMEM
    scratch = dict(
        fetch=pltpu.SemaphoreType.DMA((4,)),
        tok_v=vmem((count, win, dim), BF16),
        cot_v=vmem((count, win, dim), BF16),
        w_qkv_v=vmem((dim, 3 * dim), BF16),
        w_proj_v=vmem((dim, dim), BF16),
        flat=vmem((dim // 128, rows, 128), F32),
        x=vmem((rows, dim), BF16),
        xt=vmem((dim, rows), BF16),
        c=vmem((rows, dim), BF16),
        qkv=vmem((rows, 3 * dim), BF16),
        d_att=vmem((rows, dim), BF16),
        att=vmem((rows, dim), BF16),
        d_v=vmem((rows, dim), BF16),
        d_qk=vmem((rows, 2 * wide), BF16),
        probs=vmem((groups, rows, GROUP * PAD), BF16),
        masks=vmem((rows, 128), F32),
        bias=vmem((groups, PAD, GROUP * PAD), F32),
        bias_rows=vmem((PAD * heads, 128), F32),
        d_bias=vmem((groups, PAD, GROUP * PAD), F32),
        small=vmem((128, 128), F32),
        rel_t=vmem((128, 128), F32),
        tab=vmem((heads, size), F32),
    )
    params = dict()
    if remote:
        chunks = dict(v=dim, p=dim) | {f"k{g}": 2 * wide for g in range(groups)}
        for name, cols in chunks.items():
            scratch[f"{name}_buf"] = vmem((2, 2, 2, 2, 4, 8, cols), F32)
            scratch[f"{name}_r0"] = vmem((2, 2, 2, 4, 8, cols), F32)
            scratch[f"{name}_r1"] = vmem((2, 2, 4, 8, cols), F32)
            scratch[f"{name}_r2"] = vmem((2, 4, 8, cols), F32)
            scratch[f"{name}_s2"] = vmem((4, 2, 8, cols), F32)
            scratch[f"{name}_r3"] = vmem((3, 2, 8, cols), F32)
        for name, lead in dict(t0=(), r0=(), t1=(), r1=(3,), r2=(4,)).items():
            scratch[f"t_{name}"] = vmem((*lead, heads, size), F32)
        scratch["send"] = pltpu.SemaphoreType.DMA((len(chunks) + 1, COPIES))
        scratch["recv"] = pltpu.SemaphoreType.DMA((len(chunks) + 1, COPIES))
        params = dict(collective_id=0, has_side_effects=True)
    dims = (win, count, dim, heads, entries, remote, norm)
    spec = pl.BlockSpec(memory_space=pltpu.VMEM)
    where = {n: pl.BlockSpec(memory_space=pl.ANY) for n in ("tok", "cot", "w_qkv", "w_proj")}
    return pl.pallas_call(
        functools.partial(kernel, dims, [*inputs, *outs, *scratch]),
        out_shape=[jax.ShapeDtypeStruct(o, F32) for o in outs.values()],
        in_specs=[where.get(n, spec) for n in inputs],
        out_specs=[spec] * len(outs),
        scratch_shapes=list(scratch.values()),
        compiler_params=pltpu.CompilerParams(vmem_limit_bytes=60 * 1024 * 1024, **params),
    )(*inputs.values())


def body(
    tokens, cotangent, regions, rel_index, w_qkv, w_proj, bias_table, mom_qkv, mom_proj, mom_table
):
    dim = tokens.shape[2]
    devices = lax.axis_size(AXES)
    sizes = tuple(lax.axis_size(a) for a in AXES)
    norm = 1.0 / (tokens.shape[0] * devices)
    args = (tokens, cotangent, regions, rel_index, w_qkv, w_proj, bias_table)
    moms = (mom_qkv, mom_proj, mom_table)
    if sizes == (2, 4, 4) and dim == 16 * devices:
        qkv, proj, table = local_grads(True, norm, *args, moms)
        return qkv.reshape(-1), proj.reshape(-1), table.T
    qkv, proj, table = local_grads(False, norm, *args, None)
    qkv_mine = lax.psum_scatter(qkv.reshape(-1), AXES, tiled=True)
    proj_mine = lax.psum_scatter(proj.reshape(-1), AXES, tiled=True)
    table = lax.psum(table, AXES)
    return (
        0.9 * mom_qkv + qkv_mine * norm,
        0.9 * mom_proj + proj_mine * norm,
        0.9 * mom_table + table.T * norm,
    )


def solution(mesh):
    return jax.shard_map(
        body,
        mesh=mesh,
        in_specs=(
            P(AXES, None, None),
            P(AXES, None, None),
            P(AXES, None),
            P(),
            P(),
            P(),
            P(),
            P(AXES),
            P(AXES),
            P(),
        ),
        out_specs=(P(AXES), P(AXES), P()),
        check_vma=False,
    )
```

```python
import functools
import math

import jax
import jax.numpy as jnp
from jax import lax
from jax.experimental import pallas as pl
from jax.experimental.pallas import tpu as pltpu
from jax.sharding import PartitionSpec as P

AXES = ("gx", "gy", "gz")
MESH = pl.DeviceIdType.MESH
F32, BF16 = jnp.float32, jnp.bfloat16
PAD = 64
GROUP = 4
BATCH = 4
LOG2E = math.log2(math.e)
NT = (((1,), (1,)), ((), ()))
TN = (((0,), (0,)), ((), ()))
COPIES = 8
SPEED = (680e3, 98e3, 98e3, 98e3)
DELAY = (1.4, 3.0, 2.6, 4.0)


class Clock:
    def __init__(self):
        self.now, self.free = 0.0, dict(core=0.0, xy=0.0, z=0.0)

    def arrival(self, stage, size):
        link = ("core", "xy", "xy", "z")[stage]
        done = max(self.now, self.free[link]) + size / SPEED[stage]
        self.free[link] = done
        return done + DELAY[stage]


def dot(a, b, dims=(((1,), (0,)), ((), ()))):
    return lax.dot_general(a, b, dims, preferred_element_type=F32)


def spread(value, lanes, width):
    return jnp.concatenate(
        [jnp.where(lanes // width == h, value, jnp.zeros_like(value)) for h in range(GROUP)], axis=0
    )


def gather_heads(value, lanes, width):
    total = jnp.where(lanes // width == 0, value[:PAD], 0.0)
    for h in range(1, GROUP):
        total = jnp.where(lanes // width == h, value[h * PAD : (h + 1) * PAD], total)
    return total


class Place:
    def __init__(self):
        gx, gy, gz = (lax.axis_index(a) for a in AXES)
        self.x, self.z = gx, gy
        self.core, self.y = gz % 2, gz // 2
        self.to_core = (gx, gy, gz + 1 - 2 * self.core)
        self.to_x = (1 - gx, gy, gz)
        self.to_y = (gx, gy, gz + 2 - 4 * self.y)
        self.to_xy = (1 - gx, gy, gz + 2 - 4 * self.y)
        self.others = [(gy + k) % 4 for k in range(1, 4)]
        self.to_z = [(gx, there, gz) for there in self.others]

    def everyone(self):
        return [self.to_core, self.to_x, self.to_y, self.to_xy, *self.to_z]


class Chunk:
    def __init__(self, place, refs, send, recv, clock, finish):
        self.p, self.clock = place, clock
        self.buf, self.r0, self.r1, self.r2, self.s2, self.r3 = refs
        self.send, self.recv, self.finish = send, recv, finish
        self.ab = ((place.x, place.y), (place.y, place.x))
        self.via = ((place.to_x, place.to_y), (place.to_y, place.to_x))
        self.stage, self.due = 0, None
        whole = 4 * math.prod(self.buf.shape)
        self.sizes = (whole / 2, whole / 4, whole / 8, whole / 4)

    def copy(self, n, src, dst, there):
        return pltpu.make_async_remote_copy(
            src_ref=src,
            dst_ref=dst,
            send_sem=self.send.at[n],
            recv_sem=self.recv.at[n],
            device_id=there,
            device_id_type=MESH,
        )

    def copies(self, stage):
        p, buf = self.p, self.buf
        if stage == 0:
            return [self.copy(0, buf.at[1 - p.core], self.r0, p.to_core)]
        if stage == 1:
            return [
                self.copy(1 + h, buf.at[p.core, h, 1 - self.ab[h][0]], self.r1.at[h], self.via[h][0])
                for h in range(2)
            ]
        if stage == 2:
            return [
                self.copy(
                    3 + h,
                    buf.at[p.core, h, self.ab[h][0], 1 - self.ab[h][1]],
                    self.r2.at[h],
                    self.via[h][1],
                )
                for h in range(2)
            ]
        return [self.copy(5 + k, self.s2.at[p.others[k]], self.r3.at[k], p.to_z[k]) for k in range(3)]

    def start(self):
        for c in self.copies(0):
            c.start()
        self.due = self.clock.arrival(0, self.sizes[0])

    def advance(self):
        p, buf, stage = self.p, self.buf, self.stage
        waited = self.copies(stage)
        after = self.copies(stage + 1) if stage < 3 else []
        if stage == 0:
            waited[0].wait()
            for h in range(2):
                away = 1 - self.ab[h][0]
                at = (p.core, h, away)
                buf[at] = buf[at] + self.r0[h, away]
                after[h].start()
        elif stage == 1:
            for h in range(2):
                a, b = self.ab[h]
                waited[h].wait()
                at = (p.core, h, a, 1 - b)
                buf[at] = buf[at] + self.r0[h, a, 1 - b] + self.r1[h, 1 - b]
                after[h].start()
        elif stage == 2:
            for h in range(2):
                a, b = self.ab[h]
                waited[h].wait()
                self.s2[:, h] = (
                    buf[p.core, h, a, b] + self.r0[h, a, b] + self.r1[h, b] + self.r2[h]
                )
            for c in after:
                c.start()
        else:
            for c in waited:
                c.wait()
            self.finish(self.s2[p.z] + self.r3[0] + self.r3[1] + self.r3[2])
        self.stage += 1
        if self.stage < 4:
            self.due = self.clock.arrival(self.stage, self.sizes[self.stage])


class Table:
    def __init__(self, place, refs, send, recv, clock, finish):
        self.p, self.clock = place, clock
        self.t0, self.r0, self.t1, self.r1, self.r2 = refs
        self.send, self.recv, self.finish = send, recv, finish
        self.stage, self.due, self.size = 1, None, 4 * math.prod(self.t0.shape)

    def copy(self, n, src, dst, there):
        return pltpu.make_async_remote_copy(
            src_ref=src,
            dst_ref=dst,
            send_sem=self.send.at[n],
            recv_sem=self.recv.at[n],
            device_id=there,
            device_id_type=MESH,
        )

    def copies(self, stage):
        p = self.p
        if stage == 1:
            return [self.copy(0, self.t0, self.r0, p.to_core)]
        if stage == 2:
            return [
                self.copy(1 + k, self.t1, self.r1.at[k], there)
                for k, there in enumerate((p.to_x, p.to_y, p.to_xy))
            ]
        return [self.copy(4 + k, self.r2.at[p.z], self.r2.at[p.z], p.to_z[k]) for k in range(3)]

    def start(self):
        for c in self.copies(1):
            c.start()
        self.due = self.clock.now + 1.5

    def advance(self):
        for c in self.copies(self.stage):
            if self.stage < 3:
                c.wait()
            else:
                c.wait_send()
        if self.stage == 1:
            self.t1[...] = self.t0[...] + self.r0[...]
        elif self.stage == 2:
            self.r2[self.p.z] = (self.t1[...] + self.r1[0]) + (self.r1[1] + self.r1[2])
        else:
            for k in range(3):
                there = (self.p.z + 3 - k) % 4
                self.copy(4 + k, self.r2.at[there], self.r2.at[there], self.p.to_z[k]).wait_recv()
            self.finish((self.r2[0] + self.r2[1]) + (self.r2[2] + self.r2[3]))
        if self.stage < 3:
            for c in self.copies(self.stage + 1):
                c.start()
            self.due = self.clock.arrival(self.stage, 4 * self.size) + 0.5
        self.stage += 1


def kernel(dims, names, *all_refs):
    win, count, dim, heads, entries, remote = dims
    r = dict(zip(names, all_refs, strict=True))
    width = dim // heads
    groups = heads // GROUP
    wide = GROUP * width
    scale = width**-0.5
    x, xt, c, qkv, d_att, att_t = r["x"], r["xt"], r["c"], r["qkv"], r["d_att"], r["att_t"]
    d_v, d_qk, probs, masks = r["d_v"], r["d_qk"], r["probs"], r["masks"]
    bias, bias_rows, d_bias, small, rel_t, tab = (
        r[n] for n in ("bias", "bias_rows", "d_bias", "small", "rel_t", "tab")
    )
    fetch = {}
    for n, name in enumerate(n[:-3] for n in names if n.endswith("_vm")):
        fetch[name] = pltpu.make_async_copy(r[name], r[f"{name}_vm"], r["fetch"].at[n])
        fetch[name].start()
    w_qkv, w_proj = r["w_qkv_vm"], r["w_proj_vm"]

    if remote:
        place = Place()
        barrier = pltpu.get_barrier_semaphore()
        for there in place.everyone():
            pl.semaphore_signal(barrier, inc=1, device_id=there, device_id_type=MESH)

    lanes = lax.broadcasted_iota(jnp.int32, (PAD, wide), 1)

    for name in ("reg", "rel", "table"):
        fetch[name].wait()
    small[...] = jnp.zeros_like(small)
    small[0:win, 0:count] = r["reg_vm"][...].astype(F32)
    reg_rows = small[...]
    reg_cols = reg_rows.T
    for w in range(win):
        row = reg_rows[w : w + 1, :PAD]
        row = jnp.concatenate([row, row], axis=1)
        masks[w * PAD : (w + 1) * PAD, :] = jnp.where(
            reg_cols[:PAD, w : w + 1] == row, 0.0, -100.0 * LOG2E
        )

    small[...] = jnp.full_like(small, -1.0)
    small[0:count, 0:count] = r["rel_vm"][...].astype(F32)
    rel_t[...] = small[...].T
    tab[...] = jnp.zeros_like(tab)
    tab[:, 0:entries] = r["table_vm"][...]
    size = tab.shape[1]
    tab_t = tab[...]
    high = tab_t.astype(BF16)
    low = (tab_t - high.astype(F32)).astype(BF16)
    both = jnp.concatenate([high, low], axis=0)
    entry = lax.broadcasted_iota(jnp.int32, (size, 128), 0).astype(F32)
    unroll = next(u for u in (7, 8, 4, 2, 1) if count % u == 0)

    def one_hot(j):
        return jnp.where(entry == rel_t[pl.ds(j, 1), :], 1.0, 0.0).astype(BF16)

    bias_rows[...] = jnp.full_like(bias_rows, -1e30)

    def look(i, carry):
        for u in range(unroll):
            j = i * unroll + u
            found = dot(both, one_hot(j))
            bias_rows[pl.ds(pl.multiple_of(j * heads, heads), heads), :] = (
                found[:heads] + found[heads:]
            ) * LOG2E
        return carry

    lax.fori_loop(0, count // unroll, look, 0)
    for g in range(groups):
        bias[g] = jnp.concatenate(
            [bias_rows[pl.ds(g * GROUP + h, PAD, stride=heads), :][:, :PAD] for h in range(GROUP)],
            axis=1,
        )
    d_bias[...] = jnp.zeros_like(d_bias)

    flat = r["flat"]
    rows_all = win * PAD
    for n in range(dim // 128):
        flat[n, count * win :, :] = jnp.zeros((rows_all - count * win, 128), F32)

    def by_window(src, dst):
        for n in range(dim // 128):
            cols = slice(n * 128, n * 128 + 128)
            for t in range(count):
                flat[n, t * win : (t + 1) * win, :] = src[t, :, cols].astype(F32)
            for w in range(win):
                dst[w * PAD : (w + 1) * PAD, cols] = flat[n, pl.ds(w, PAD, stride=win), :].astype(BF16)

    fetch["tok"].wait()
    by_window(r["tok_vm"], x)
    fetch["cot"].wait()
    by_window(r["cot_vm"], c)
    fetch["w_qkv"].wait()
    fetch["w_proj"].wait()

    def project(n):
        half = dim // 2

        @pl.loop(0, rows_all // 256)
        def _(i):
            rows = pl.ds(pl.multiple_of(i * 256, 256), 256)
            for which in range(3):
                cols = slice(which * dim + n * half, which * dim + (n + 1) * half)
                qkv[rows, cols] = dot(x[rows, :], w_qkv[:, cols]).astype(BF16)
            cols = slice(n * half, (n + 1) * half)
            d_att[rows, cols] = dot(c[rows, :], w_proj[cols, :], NT).astype(BF16)

    project(0)
    xt[...] = x[...].T

    def rows_of(w):
        at = w * PAD
        return pl.ds(at if isinstance(at, int) else pl.multiple_of(at, PAD), PAD)

    def part(ref, which, g, rows):
        at = which * dim + g * wide
        return ref[rows, at : at + wide]

    ring, ring_ds = r["ring"], r["ring_ds"]

    def pipelined(batches, stages, after):
        for s in range(len(batches) + len(stages) - 1):
            for k in reversed(range(len(stages))):
                if 0 <= s - k < len(batches):
                    stages[k](batches[s - k], (s - k) % 2 * BATCH)
            after(s - len(stages) + 1)

    def get_scores(units, at):
        for n, (g, w) in enumerate(units):
            rows = rows_of(w)
            query = spread(part(qkv, 0, g, rows), lanes, width)
            ring[at + n] = dot(part(qkv, 1, g, rows), query, NT)

    def get_probs(units, at):
        for n, (g, w) in enumerate(units):
            rows = rows_of(w)
            mask = jnp.concatenate([masks[rows, :]] * (GROUP * PAD // 128), axis=1)
            v = ring[at + n] * (scale * LOG2E) + bias[g] + mask
            v = jnp.exp2(v - jnp.max(v, axis=0, keepdims=True))
            probs[g, rows, :] = (v * (1.0 / jnp.sum(v, axis=0, keepdims=True))).astype(BF16)

    def use_probs(units, at):
        for g, w in units:
            rows = rows_of(w)
            p = probs[g, rows, :]
            mixed = dot(part(qkv, 2, g, rows), p, TN).astype(BF16)
            for h in range(GROUP):
                att_t[g * wide + h * width : g * wide + (h + 1) * width, rows] = mixed[
                    h * width : (h + 1) * width, h * PAD : (h + 1) * PAD
                ]
            d_out = spread(part(d_att, 0, g, rows), lanes, width)
            d_v[rows, g * wide : (g + 1) * wide] = dot(p, d_out).astype(BF16)

    clock = Clock()
    active = []

    def put(value, ref):
        for d in range(value.shape[0] // 16):
            dx, dz, dy, dc = d // 16, (d // 4) % 4, (d // 2) % 2, d % 2
            for half in range(2):
                a, b = (dx, dy) if half == 0 else (dy, dx)
                ref[dc, half, a, b, dz] = value[16 * d + 8 * half : 16 * d + 8 * half + 8]

    def update(out, at, tiles, value):
        for half in range(2):
            for n in range(value.shape[2] // 128):
                rows = pl.ds(half * 8 * tiles + at(n), 8, stride=tiles)
                out[rows, :] = value[half, :, n * 128 : n * 128 + 128]

    def ship(name, n, value, finish):
        refs = [r[f"{name}_{k}"] for k in ("buf", "r0", "r1", "r2", "s2", "r3")]
        put(value, refs[0])
        chunk = Chunk(place, refs, r["send"].at[n], r["recv"].at[n], clock, finish)
        chunk.start()
        active.append(chunk)

    def run_due(passed, last=False):
        clock.now += passed
        while True:
            ready = [k for k in active if k.stage < 4 and (last or k.stage < 3 and k.due <= clock.now)]
            if not ready:
                return
            first = min(ready, key=lambda k: (k.stage == 3, k.due))
            clock.now = max(clock.now, first.due)
            first.advance()

    if remote:
        pl.semaphore_wait(barrier, len(place.everyone()))
    tiles = dim // 128
    per = wide // 128
    half = dim // 2
    pairs = groups // 2
    for n in range(pairs):
        units = [(g, w) for w in range(win) for g in (2 * n, 2 * n + 1)]
        batches = [units[k : k + BATCH] for k in range(0, len(units), BATCH)]

        def after(done):
            if remote and done % 2 == 1:
                run_due(0.45)

        if n:
            project(n)
            if remote:
                run_due(1.4)
        pipelined(batches, (get_scores, get_probs, use_probs), after)
        cols = slice(2 * n * wide, 2 * (n + 1) * wide)
        g_v = dot(xt[...], d_v[:, cols])
        if remote:
            at = lambda k, n=n: 2 * tiles + 2 * n * per + k
            ship(f"v{n}", n, g_v, functools.partial(update, r["out_qkv"], at, 3 * tiles))
            run_due(0.5)
        else:
            r["out_qkv"][:, 2 * dim + cols.start : 2 * dim + cols.stop] = g_v
    for n in range(2):
        cols = slice(n * half, (n + 1) * half)
        g_proj = dot(att_t[...], c[:, cols])
        if remote:
            at = lambda k, n=n: n * tiles // 2 + k
            ship(f"p{n}", pairs + n, g_proj, functools.partial(update, r["out_proj"], at, tiles))
            run_due(0.6)
        else:
            r["out_proj"][:, cols] = g_proj

    def get_d_probs(units, at):
        for n, (g, w) in enumerate(units):
            rows = rows_of(w)
            d_out = spread(part(d_att, 0, g, rows), lanes, width)
            ring[at + n] = dot(part(qkv, 2, g, rows), d_out, NT)

    def get_d_scores(units, at):
        g = units[0][0]
        total = d_bias[g]
        for n, (_, w) in enumerate(units):
            pf = probs[g, rows_of(w), :].astype(F32)
            weighted = pf * ring[at + n]
            ds = weighted - pf * jnp.sum(weighted, axis=0, keepdims=True)
            total = total + ds
            ring_ds[at + n] = ds.astype(BF16)
        d_bias[g] = total

    def use_d_scores(units, at):
        for n, (g, w) in enumerate(units):
            rows = rows_of(w)
            ds = ring_ds[at + n]
            d_k = dot(ds, spread(part(qkv, 0, g, rows), lanes, width)) * scale
            d_q = gather_heads(dot(ds, part(qkv, 1, g, rows), TN), lanes, width) * scale
            d_qk[g % 2, rows, :] = jnp.concatenate([d_q, d_k], axis=1).astype(BF16)

    def send_qk(g):
        g_qk = dot(xt[...], d_qk[g % 2])
        if remote:
            at = lambda n, g=g: (n // per) * tiles + g * per + n % per
            ship(f"k{g}", pairs + 2 + g, g_qk, functools.partial(update, r["out_qkv"], at, 3 * tiles))
            run_due(0.5)
        else:
            for which in range(2):
                at = which * dim + g * wide
                r["out_qkv"][:, at : at + wide] = g_qk[:, which * wide : (which + 1) * wide]


    units = [(g, w) for g in range(groups) for w in range(win)]
    batches = [units[k : k + BATCH] for k in range(0, len(units), BATCH)]

    def after_backward(done):
        if remote and done % 2 == 0:
            run_due(0.6)
        if done >= 0 and (done + 1) * BATCH % win == 0:
            send_qk(batches[done][0][0])

    pipelined(batches, (get_d_probs, get_d_scores, use_d_scores), after_backward)

    for g in range(groups):
        for h in range(GROUP):
            piece = d_bias[g, :, h * PAD : (h + 1) * PAD]
            bias_rows[pl.ds(g * GROUP + h, PAD, stride=heads), :] = jnp.concatenate(
                [piece, jnp.zeros_like(piece)], axis=1
            )

    def collect(i, total):
        for u in range(unroll):
            j = i * unroll + u
            value = bias_rows[pl.ds(pl.multiple_of(j * heads, heads), heads), :]
            top = value.astype(BF16)
            rest_of = (value - top.astype(F32)).astype(BF16)
            total = total + dot(jnp.concatenate([top, rest_of], axis=0), one_hot(j), NT)
        return total

    if remote:
        run_due(0.3)
    g_table = jnp.zeros((2 * heads, size), F32)
    steps = count // unroll
    for k in range(2):
        g_table = lax.fori_loop(k * steps // 2, (k + 1) * steps // 2, collect, g_table)
        if remote:
            run_due(0.9)
    g_table = g_table[:heads] + g_table[heads:]
    if not remote:
        r["out_table"][...] = g_table[:, :entries]
        return
    refs = [r[f"t_{k}"] for k in ("t0", "r0", "t1", "r1", "r2")]
    refs[0][...] = g_table

    def table_done(value):
        r["out_table"][...] = value[:, :entries]

    n = pairs + 2 + groups
    last = Table(place, refs, r["send"].at[n], r["recv"].at[n], clock, table_done)
    last.start()
    active.append(last)
    run_due(0.0, True)


def local_grads(remote, tokens, cotangent, regions, rel_index, w_qkv, w_proj, bias_table):
    win, count, dim = tokens.shape
    entries, heads = bias_table.shape
    groups = heads // GROUP
    rows = win * PAD
    wide = GROUP * (dim // heads)
    size = -(-entries // 128) * 128
    own = dim // 32
    inputs = dict(
        reg=regions,
        rel=rel_index,
        table=bias_table.T,
        tok=tokens.transpose(1, 0, 2),
        w_qkv=w_qkv,
        cot=cotangent.transpose(1, 0, 2),
        w_proj=w_proj,
    )
    if remote:
        outs = dict(
            out_qkv=(own * 3 * dim // 128, 128), out_proj=(own * dim // 128, 128), out_table=(heads, entries)
        )
    else:
        outs = dict(out_qkv=(dim, 3 * dim), out_proj=(dim, dim), out_table=(heads, entries))
    vmem = pltpu.VMEM
    scratch = {f"{n}_vm": vmem(v.shape, v.dtype) for n, v in inputs.items()}
    scratch |= dict(
        fetch=pltpu.SemaphoreType.DMA((len(inputs),)),
        flat=vmem((dim // 128, rows, 128), F32),
        x=vmem((rows, dim), BF16),
        xt=vmem((dim, rows), BF16),
        c=vmem((rows, dim), BF16),
        qkv=vmem((rows, 3 * dim), BF16),
        d_att=vmem((rows, dim), BF16),
        att_t=vmem((dim, rows), BF16),
        d_v=vmem((rows, dim), BF16),
        d_qk=vmem((2, rows, 2 * wide), BF16),
        ring=vmem((2 * BATCH, PAD, GROUP * PAD), F32),
        ring_ds=vmem((2 * BATCH, PAD, GROUP * PAD), BF16),
        probs=vmem((groups, rows, GROUP * PAD), BF16),
        masks=vmem((rows, 128), F32),
        bias=vmem((groups, PAD, GROUP * PAD), F32),
        bias_rows=vmem((PAD * heads, 128), F32),
        d_bias=vmem((groups, PAD, GROUP * PAD), F32),
        small=vmem((128, 128), F32),
        rel_t=vmem((128, 128), F32),
        tab=vmem((heads, size), F32),
    )
    params = dict()
    if remote:
        chunks = {f"v{n}": 2 * wide for n in range(groups // 2)} | dict(p0=dim // 2, p1=dim // 2)
        chunks |= {f"k{g}": 2 * wide for g in range(groups)}
        for name, cols in chunks.items():
            scratch[f"{name}_buf"] = vmem((2, 2, 2, 2, 4, 8, cols), F32)
            scratch[f"{name}_r0"] = vmem((2, 2, 2, 4, 8, cols), F32)
            scratch[f"{name}_r1"] = vmem((2, 2, 4, 8, cols), F32)
            scratch[f"{name}_r2"] = vmem((2, 4, 8, cols), F32)
            scratch[f"{name}_s2"] = vmem((4, 2, 8, cols), F32)
            scratch[f"{name}_r3"] = vmem((3, 2, 8, cols), F32)
        for name, lead in dict(t0=(), r0=(), t1=(), r1=(3,), r2=(4,)).items():
            scratch[f"t_{name}"] = vmem((*lead, heads, size), F32)
        scratch["send"] = pltpu.SemaphoreType.DMA((len(chunks) + 1, COPIES))
        scratch["recv"] = pltpu.SemaphoreType.DMA((len(chunks) + 1, COPIES))
        params = dict(collective_id=0, has_side_effects=True)
    dims = (win, count, dim, heads, entries, remote)
    spec = pl.BlockSpec(memory_space=pltpu.VMEM)
    return pl.pallas_call(
        functools.partial(kernel, dims, [*inputs, *outs, *scratch]),
        out_shape=[jax.ShapeDtypeStruct(o, F32) for o in outs.values()],
        in_specs=[pl.BlockSpec(memory_space=pl.ANY)] * len(inputs),
        out_specs=[spec] * len(outs),
        scratch_shapes=list(scratch.values()),
        compiler_params=pltpu.CompilerParams(vmem_limit_bytes=60 * 1024 * 1024, **params),
    )(*inputs.values())


def momentum_kernel(norm, *refs):
    for grad, old, new in zip(refs[:3], refs[3:6], refs[6:], strict=True):
        new[...] = 0.9 * old[...] + grad[...] * norm


def momentum(norm, grads, moms):
    old = [m.reshape(g.shape) if m.ndim == 1 else m.T for g, m in zip(grads, moms, strict=True)]
    spec = pl.BlockSpec(memory_space=pltpu.VMEM)
    return pl.pallas_call(
        functools.partial(momentum_kernel, norm),
        out_shape=[jax.ShapeDtypeStruct(g.shape, F32) for g in grads],
        in_specs=[spec] * 6,
        out_specs=[spec] * 3,
    )(*grads, *old)


def body(
    tokens, cotangent, regions, rel_index, w_qkv, w_proj, bias_table, mom_qkv, mom_proj, mom_table
):
    dim = tokens.shape[2]
    devices = lax.axis_size(AXES)
    sizes = tuple(lax.axis_size(a) for a in AXES)
    norm = 1.0 / (tokens.shape[0] * devices)
    args = (tokens, cotangent, regions, rel_index, w_qkv, w_proj, bias_table)
    if sizes == (2, 4, 4) and dim == 16 * devices:
        grads = local_grads(True, *args)
        qkv, proj, table = momentum(norm, grads, (mom_qkv, mom_proj, mom_table))
        return qkv.reshape(-1), proj.reshape(-1), table.T
    qkv, proj, table = local_grads(False, *args)
    qkv_mine = lax.psum_scatter(qkv.reshape(-1), AXES, tiled=True)
    proj_mine = lax.psum_scatter(proj.reshape(-1), AXES, tiled=True)
    table = lax.psum(table, AXES)
    return (
        0.9 * mom_qkv + qkv_mine * norm,
        0.9 * mom_proj + proj_mine * norm,
        0.9 * mom_table + table.T * norm,
    )


def solution(mesh):
    return jax.shard_map(
        body,
        mesh=mesh,
        in_specs=(
            P(AXES, None, None),
            P(AXES, None, None),
            P(AXES, None),
            P(),
            P(),
            P(),
            P(),
            P(AXES),
            P(AXES),
            P(),
        ),
        out_specs=(P(AXES), P(AXES), P()),
        check_vma=False,
    )
```

```python
import functools
import math

import jax
import jax.numpy as jnp
from jax import lax
from jax.experimental import pallas as pl
from jax.experimental.pallas import tpu as pltpu
from jax.sharding import PartitionSpec as P

AXES = ("gx", "gy", "gz")
MESH = pl.DeviceIdType.MESH
F32, BF16 = jnp.float32, jnp.bfloat16
PAD = 64
GROUP = 4
BATCH = 4
MSPLIT = 2
LOG2E = math.log2(math.e)
NT = (((1,), (1,)), ((), ()))
TN = (((0,), (0,)), ((), ()))
COPIES = 8
SPEED = dict(core=680e3, xy=98e3, z=98e3)
DELAY = dict(core=1.4, xy=2.4, z=4.0)


def tall_dot(a, b):
    step = a.shape[0] // MSPLIT
    return jnp.concatenate([dot(a[k * step : (k + 1) * step, :], b) for k in range(MSPLIT)], axis=0)


class Clock:
    def __init__(self):
        self.now, self.free = 0.0, dict(core=0.0, xy=0.0, z=0.0)

    def arrival(self, link, size):
        done = max(self.now, self.free[link]) + size / SPEED[link]
        self.free[link] = done
        return done + DELAY[link]


def dot(a, b, dims=(((1,), (0,)), ((), ()))):
    return lax.dot_general(a, b, dims, preferred_element_type=F32)


def spread(value, lanes, width):
    return jnp.concatenate(
        [jnp.where(lanes // width == h, value, jnp.zeros_like(value)) for h in range(GROUP)], axis=0
    )


def gather_heads(value, lanes, width):
    total = jnp.where(lanes // width == 0, value[:PAD], 0.0)
    for h in range(1, GROUP):
        total = jnp.where(lanes // width == h, value[h * PAD : (h + 1) * PAD], total)
    return total


class Place:
    def __init__(self):
        gx, gy, gz = (lax.axis_index(a) for a in AXES)
        self.x, self.z = gx, gy
        self.core, self.y = gz % 2, gz // 2
        self.to_core = (gx, gy, gz + 1 - 2 * self.core)
        self.to_x = (1 - gx, gy, gz)
        self.to_y = (gx, gy, gz + 2 - 4 * self.y)
        self.to_xy = (1 - gx, gy, gz + 2 - 4 * self.y)
        self.others = [(gy + k) % 4 for k in range(1, 4)]
        self.to_z = [(gx, there, gz) for there in self.others]

    def everyone(self):
        return [self.to_core, self.to_x, self.to_y, self.to_xy, *self.to_z]


class Chunk:
    links = ("core", "xy", "xy", "z")

    def set_sizes(self, whole):
        self.sizes = (whole / 2, whole / 4, whole / 8, whole / 4)

    def __init__(self, place, refs, send, recv, clock, finish):
        self.p, self.clock = place, clock
        self.buf, self.r0, self.r1, self.r2, self.s2, self.r3 = refs
        self.send, self.recv, self.finish = send, recv, finish
        self.ab = ((place.x, place.y), (place.y, place.x))
        self.via = ((place.to_x, place.to_y), (place.to_y, place.to_x))
        self.stage, self.due = 0, None
        self.set_sizes(4 * math.prod(self.buf.shape))

    def copy(self, n, src, dst, there):
        return pltpu.make_async_remote_copy(
            src_ref=src,
            dst_ref=dst,
            send_sem=self.send.at[n],
            recv_sem=self.recv.at[n],
            device_id=there,
            device_id_type=MESH,
        )

    def copies(self, stage):
        p, buf = self.p, self.buf
        if stage == 0:
            return [self.copy(0, buf.at[1 - p.core], self.r0, p.to_core)]
        if stage == 1:
            return [
                self.copy(1 + h, buf.at[p.core, h, 1 - self.ab[h][0]], self.r1.at[h], self.via[h][0])
                for h in range(2)
            ]
        if stage == 2:
            return [
                self.copy(
                    3 + h,
                    buf.at[p.core, h, self.ab[h][0], 1 - self.ab[h][1]],
                    self.r2.at[h],
                    self.via[h][1],
                )
                for h in range(2)
            ]
        return [self.copy(5 + k, self.s2.at[p.others[k]], self.r3.at[k], p.to_z[k]) for k in range(3)]

    def final(self):
        return self.stage == 3

    def start(self):
        for c in self.copies(0):
            c.start()
        self.due = self.clock.arrival("core", self.sizes[0])

    def advance(self):
        p, buf, stage = self.p, self.buf, self.stage
        waited = self.copies(stage)
        after = self.copies(stage + 1) if stage < 3 else []
        if stage == 0:
            waited[0].wait()
            for h in range(2):
                away = 1 - self.ab[h][0]
                at = (p.core, h, away)
                buf[at] = buf[at] + self.r0[h, away]
                after[h].start()
        elif stage == 1:
            for h in range(2):
                a, b = self.ab[h]
                waited[h].wait()
                at = (p.core, h, a, 1 - b)
                buf[at] = buf[at] + self.r0[h, a, 1 - b] + self.r1[h, 1 - b]
                after[h].start()
        elif stage == 2:
            for h in range(2):
                a, b = self.ab[h]
                waited[h].wait()
                self.s2[:, h] = (
                    buf[p.core, h, a, b] + self.r0[h, a, b] + self.r1[h, b] + self.r2[h]
                )
            for c in after:
                c.start()
        else:
            for c in waited:
                c.wait()
            done = self.s2[p.z] + self.r3[0] + self.r3[1] + self.r3[2]
            self.finish([done[0], done[1]])
        self.stage += 1
        if self.stage < 4:
            self.due = self.clock.arrival(self.links[self.stage], self.sizes[self.stage])


class ChunkZ(Chunk):
    links = ("core", "z", "xy", "xy")

    def set_sizes(self, whole):
        self.sizes = (whole / 2, whole, whole / 16, whole / 32)

    def copies(self, stage):
        p, buf = self.p, self.buf
        if stage == 0:
            return [self.copy(0, buf.at[1 - p.core], self.r0, p.to_core)]
        if stage == 1:
            return [self.copy(1 + k, buf.at[p.core, p.others[k]], self.r1.at[k], p.to_z[k]) for k in range(3)]
        if stage == 2:
            return [
                self.copy(4 + h, self.s2.at[h, 1 - self.ab[h][0]], self.r2.at[h], self.via[h][0])
                for h in range(2)
            ]
        return [
            self.copy(6 + h, self.s2.at[h, self.ab[h][0], 1 - self.ab[h][1]], self.r3.at[h], self.via[h][1])
            for h in range(2)
        ]

    def advance(self):
        p, buf, s2, stage = self.p, self.buf, self.s2, self.stage
        waited = self.copies(stage)
        after = self.copies(stage + 1) if stage < 3 else []
        for c in waited:
            c.wait()
        if stage == 0:
            for k, z in enumerate(p.others):
                buf[p.core, z] = buf[p.core, z] + self.r0[z]
                after[k].start()
        elif stage == 1:
            for h in range(2):
                for a in (1 - self.ab[h][0], self.ab[h][0]):
                    s2[h, a] = (buf[p.core, p.z, h, a] + self.r0[p.z, h, a]) + (
                        self.r1[0, h, a] + self.r1[1, h, a] + self.r1[2, h, a]
                    )
                after[h].start()
        elif stage == 2:
            for h in range(2):
                a = self.ab[h][0]
                s2[h, a] = s2[h, a] + self.r2[h]
                after[h].start()
        else:
            self.finish([s2[h, self.ab[h][0], self.ab[h][1]] + self.r3[h] for h in range(2)])
        self.stage += 1
        if self.stage < 4:
            self.due = self.clock.arrival(self.links[self.stage], self.sizes[self.stage])


class Table:
    def __init__(self, place, refs, send, recv, clock, finish):
        self.p, self.clock = place, clock
        self.t0, self.r0, self.t1, self.r1, self.r2, self.t3 = refs
        self.send, self.recv, self.finish = send, recv, finish
        self.stage, self.due, self.size = 0, None, 4 * math.prod(self.t1.shape)

    def copy(self, n, src, dst, there):
        return pltpu.make_async_remote_copy(
            src_ref=src,
            dst_ref=dst,
            send_sem=self.send.at[n],
            recv_sem=self.recv.at[n],
            device_id=there,
            device_id_type=MESH,
        )

    def copies(self, stage):
        p = self.p
        if stage == 0:
            return [self.copy(0, self.t0.at[1 - p.core], self.r0, p.to_core)]
        if stage == 1:
            return [
                self.copy(1 + k, self.t1, self.r1.at[k], there)
                for k, there in enumerate((p.to_x, p.to_y, p.to_xy))
            ]
        if stage == 2:
            return [self.copy(4 + k, self.r2.at[p.z], self.r2.at[p.z], p.to_z[k]) for k in range(3)]
        return [self.copy(7, self.t3.at[p.core], self.t3.at[p.core], p.to_core)]

    def final(self):
        return self.stage > 1

    def start(self):
        for c in self.copies(0):
            c.start()
        self.due = self.clock.now + 1.5

    def advance(self):
        p, stage = self.p, self.stage
        for c in self.copies(stage):
            if stage < 2:
                c.wait()
            else:
                c.wait_send()
        if stage == 0:
            self.t1[...] = self.t0[p.core] + self.r0[...]
        elif stage == 1:
            self.r2[p.z] = (self.t1[...] + self.r1[0]) + (self.r1[1] + self.r1[2])
        elif stage == 2:
            for k in range(3):
                there = (p.z + 3 - k) % 4
                self.copy(4 + k, self.r2.at[there], self.r2.at[there], p.to_z[k]).wait_recv()
            self.t3[p.core] = (self.r2[0] + self.r2[1]) + (self.r2[2] + self.r2[3])
        else:
            self.copy(7, self.t3.at[1 - p.core], self.t3.at[1 - p.core], p.to_core).wait_recv()
            self.finish(self.t3)
        self.stage += 1
        if self.stage < 4:
            for c in self.copies(self.stage):
                c.start()
            if self.stage == 3:
                self.due = self.clock.now + 1.5
            else:
                self.due = self.clock.arrival(("xy", "z")[self.stage - 1], 4 * self.size) + (2.0 if self.stage == 1 else 0.5)


def kernel(dims, names, *all_refs):
    win, count, dim, heads, entries, remote = dims
    r = dict(zip(names, all_refs, strict=True))
    width = dim // heads
    groups = heads // GROUP
    wide = GROUP * width
    scale = width**-0.5
    x, xt, c, qkv, d_att, att_t = r["x"], r["xt"], r["c"], r["qkv"], r["d_att"], r["att_t"]
    d_v, d_qk, probs, masks = r["d_v"], r["d_qk"], r["probs"], r["masks"]
    bias, bias_rows, d_bias, small, rel_t, tab = (
        r[n] for n in ("bias", "bias_rows", "d_bias", "small", "rel_t", "tab")
    )
    fetch = {}
    for n, name in enumerate(n[:-3] for n in names if n.endswith("_vm")):
        fetch[name] = pltpu.make_async_copy(r[name], r[f"{name}_vm"], r["fetch"].at[n])
        fetch[name].start()
    w_qkv, w_proj = r["w_qkv_vm"], r["w_proj_vm"]

    if remote:
        place = Place()
        barrier = pltpu.get_barrier_semaphore()
        for there in place.everyone():
            pl.semaphore_signal(barrier, inc=1, device_id=there, device_id_type=MESH)

    lanes = lax.broadcasted_iota(jnp.int32, (PAD, wide), 1)

    for name in ("reg", "rel", "table"):
        fetch[name].wait()
    small[...] = jnp.zeros_like(small)
    small[0:win, 0:count] = r["reg_vm"][...].astype(F32)
    reg_rows = small[...]
    reg_cols = reg_rows.T
    for w in range(win):
        row = reg_rows[w : w + 1, :PAD]
        row = jnp.concatenate([row, row], axis=1)
        masks[w * PAD : (w + 1) * PAD, :] = jnp.where(
            reg_cols[:PAD, w : w + 1] == row, 0.0, -100.0 * LOG2E
        )

    small[...] = jnp.full_like(small, -1.0)
    small[0:count, 0:count] = r["rel_vm"][...].astype(F32)
    rel_t[...] = small[...].T
    tab[...] = jnp.zeros_like(tab)
    tab[:, 0:entries] = r["table_vm"][...]
    size = tab.shape[1]
    tab_t = tab[...]
    high = tab_t.astype(BF16)
    low = (tab_t - high.astype(F32)).astype(BF16)
    both = jnp.concatenate([high, low], axis=0)
    entry = lax.broadcasted_iota(jnp.int32, (size, 128), 0).astype(F32)
    unroll = next(u for u in (7, 8, 4, 2, 1) if count % u == 0)

    def one_hot(j):
        return jnp.where(entry == rel_t[pl.ds(j, 1), :], 1.0, 0.0).astype(BF16)

    bias_rows[...] = jnp.full_like(bias_rows, -1e30)

    def look(i, carry):
        for u in range(unroll):
            j = i * unroll + u
            found = dot(both, one_hot(j))
            bias_rows[j * heads : (j + 1) * heads, :] = (
                found[:heads] + found[heads:]
            ) * LOG2E
        return carry

    for i in range(count // unroll):
        look(i, 0)
    for g in range(groups):
        bias[g] = jnp.concatenate(
            [bias_rows[pl.ds(g * GROUP + h, PAD, stride=heads), :][:, :PAD] for h in range(GROUP)],
            axis=1,
        )
    d_bias[...] = jnp.zeros_like(d_bias)

    flat = r["flat"]
    rows_all = win * PAD
    for n in range(dim // 128):
        flat[n, count * win :, :] = jnp.zeros((rows_all - count * win, 128), F32)

    def by_window(src, dst):
        for n in range(dim // 128):
            cols = slice(n * 128, n * 128 + 128)
            for t in range(count):
                flat[n, t * win : (t + 1) * win, :] = src[t, :, cols].astype(F32)
            for w in range(win):
                dst[w * PAD : (w + 1) * PAD, cols] = flat[n, pl.ds(w, PAD, stride=win), :].astype(BF16)

    fetch["tok"].wait()
    by_window(r["tok_vm"], x)
    fetch["cot"].wait()
    by_window(r["cot_vm"], c)
    fetch["w_qkv"].wait()
    fetch["w_proj"].wait()

    def project(n):
        half = dim // 2

        @pl.loop(0, rows_all // 256)
        def _(i):
            rows = pl.ds(pl.multiple_of(i * 256, 256), 256)
            for which in range(3):
                cols = slice(which * dim + n * half, which * dim + (n + 1) * half)
                qkv[rows, cols] = dot(x[rows, :], w_qkv[:, cols]).astype(BF16)
            cols = slice(n * half, (n + 1) * half)
            d_att[rows, cols] = dot(c[rows, :], w_proj[cols, :], NT).astype(BF16)

    project(0)
    xt[...] = x[...].T

    def rows_of(w):
        at = w * PAD
        return pl.ds(at if isinstance(at, int) else pl.multiple_of(at, PAD), PAD)

    def part(ref, which, g, rows):
        at = which * dim + g * wide
        return ref[rows, at : at + wide]

    ring, ring_ds = r["ring"], r["ring_ds"]

    def pipelined(batches, stages, after):
        for s in range(len(batches) + len(stages) - 1):
            for k in reversed(range(len(stages))):
                if 0 <= s - k < len(batches):
                    stages[k](batches[s - k], (s - k) % 2 * BATCH)
            after(s - len(stages) + 1)

    def get_scores(units, at):
        for n, (g, w) in enumerate(units):
            rows = rows_of(w)
            query = spread(part(qkv, 0, g, rows), lanes, width)
            ring[at + n] = dot(part(qkv, 1, g, rows), query, NT)

    def get_probs(units, at):
        for n, (g, w) in enumerate(units):
            rows = rows_of(w)
            mask = jnp.concatenate([masks[rows, :]] * (GROUP * PAD // 128), axis=1)
            v = ring[at + n] * (scale * LOG2E) + bias[g] + mask
            v = jnp.exp2(v - jnp.max(v, axis=0, keepdims=True))
            probs[g, rows, :] = (v * (1.0 / jnp.sum(v, axis=0, keepdims=True))).astype(BF16)

    def use_probs(units, at):
        for g, w in units:
            rows = rows_of(w)
            p = probs[g, rows, :]
            mixed = dot(part(qkv, 2, g, rows), p, TN).astype(BF16)
            for h in range(GROUP):
                att_t[g * wide + h * width : g * wide + (h + 1) * width, rows] = mixed[
                    h * width : (h + 1) * width, h * PAD : (h + 1) * PAD
                ]
            d_out = spread(part(d_att, 0, g, rows), lanes, width)
            d_v[rows, g * wide : (g + 1) * wide] = dot(p, d_out).astype(BF16)

    clock = Clock()
    active = []

    def put(value, ref, z_first):
        for d in range(value.shape[0] // 16):
            dx, dz, dy, dc = d // 16, (d // 4) % 4, (d // 2) % 2, d % 2
            for half in range(2):
                a, b = (dx, dy) if half == 0 else (dy, dx)
                at = (dc, dz, half, a, b) if z_first else (dc, half, a, b, dz)
                ref[at] = value[16 * d + 8 * half : 16 * d + 8 * half + 8]

    def update(out, at, tiles, value):
        for half in range(2):
            for n in range(value[half].shape[1] // 128):
                rows = pl.ds(half * 8 * tiles + at(n), 8, stride=tiles)
                out[rows, :] = value[half][:, n * 128 : n * 128 + 128]

    def ship(name, n, value, finish):
        refs = [r[f"{name}_{k}"] for k in ("buf", "r0", "r1", "r2", "s2", "r3")]
        z_first = name[0] == "v"
        put(value, refs[0], z_first)
        chunk = (ChunkZ if z_first else Chunk)(place, refs, r["send"].at[n], r["recv"].at[n], clock, finish)
        chunk.start()
        active.append(chunk)

    def run_due(passed, last=False):
        clock.now += passed
        while True:
            ready = [k for k in active if k.stage < 4 and (last or k.due <= clock.now and not k.final())]
            if not ready:
                return
            first = min(ready, key=lambda k: (k.final(), k.due))
            clock.now = max(clock.now, first.due)
            first.advance()

    if remote:
        pl.semaphore_wait(barrier, len(place.everyone()))
    tiles = dim // 128
    per = wide // 128
    half = dim // 2
    pairs = groups // 2
    for n in range(pairs):
        units = [(g, w) for w in range(win) for g in (2 * n, 2 * n + 1)]
        batches = [units[k : k + BATCH] for k in range(0, len(units), BATCH)]

        def after(done):
            if remote and done % 2 == 1:
                run_due(0.45)

        if n:
            project(n)
            if remote:
                run_due(1.4)
        pipelined(batches, (get_scores, get_probs, use_probs), after)
        cols = slice(2 * n * wide, 2 * (n + 1) * wide)
        g_v = tall_dot(xt, d_v[:, cols])
        if remote:
            at = lambda k, n=n: 2 * tiles + 2 * n * per + k
            ship(f"v{n}", n, g_v, functools.partial(update, r["out_qkv"], at, 3 * tiles))
            run_due(0.5)
        else:
            r["out_qkv"][:, 2 * dim + cols.start : 2 * dim + cols.stop] = g_v
    for n in range(2):
        cols = slice(n * half, (n + 1) * half)
        g_proj = tall_dot(att_t, c[:, cols])
        if remote:
            at = lambda k, n=n: n * tiles // 2 + k
            ship(f"p{n}", pairs + n, g_proj, functools.partial(update, r["out_proj"], at, tiles))
            run_due(0.6)
        else:
            r["out_proj"][:, cols] = g_proj

    def get_d_probs(units, at):
        for n, (g, w) in enumerate(units):
            rows = rows_of(w)
            d_out = spread(part(d_att, 0, g, rows), lanes, width)
            ring[at + n] = dot(part(qkv, 2, g, rows), d_out, NT)

    def get_d_scores(units, at):
        g = units[0][0]
        total = d_bias[g]
        for n, (_, w) in enumerate(units):
            pf = probs[g, rows_of(w), :].astype(F32)
            weighted = pf * ring[at + n]
            ds = weighted - pf * jnp.sum(weighted, axis=0, keepdims=True)
            total = total + ds
            ring_ds[at + n] = ds.astype(BF16)
        d_bias[g] = total

    def use_d_scores(units, at):
        for n, (g, w) in enumerate(units):
            rows = rows_of(w)
            ds = ring_ds[at + n]
            d_k = dot(ds, spread(part(qkv, 0, g, rows), lanes, width)) * scale
            d_q = gather_heads(dot(ds, part(qkv, 1, g, rows), TN), lanes, width) * scale
            d_qk[g % 2, rows, :] = jnp.concatenate([d_q, d_k], axis=1).astype(BF16)

    def send_qk(g):
        g_qk = tall_dot(xt, d_qk[g % 2])
        if remote:
            at = lambda n, g=g: (n // per) * tiles + g * per + n % per
            ship(f"k{g}", pairs + 2 + g, g_qk, functools.partial(update, r["out_qkv"], at, 3 * tiles))
            run_due(0.5)
        else:
            for which in range(2):
                at = which * dim + g * wide
                r["out_qkv"][:, at : at + wide] = g_qk[:, which * wide : (which + 1) * wide]


    units = [(g, w) for g in range(groups) for w in range(win)]
    batches = [units[k : k + BATCH] for k in range(0, len(units), BATCH)]

    def after_backward(done):
        if remote and done % 2 == 0:
            run_due(0.6)
        if done >= 0 and (done + 1) * BATCH % win == 0:
            send_qk(batches[done][0][0])

    pipelined(batches, (get_d_probs, get_d_scores, use_d_scores), after_backward)

    for g in range(groups):
        for h in range(GROUP):
            piece = d_bias[g, :, h * PAD : (h + 1) * PAD]
            bias_rows[pl.ds(g * GROUP + h, PAD, stride=heads), :] = jnp.concatenate(
                [piece, jnp.zeros_like(piece)], axis=1
            )

    def collect(i, total):
        for u in range(unroll):
            j = i * unroll + u
            value = bias_rows[pl.ds(pl.multiple_of(j * heads, heads), heads), :]
            top = value.astype(BF16)
            rest_of = (value - top.astype(F32)).astype(BF16)
            total = total + dot(jnp.concatenate([top, rest_of], axis=0), one_hot(j), NT)
        return total

    if remote:
        run_due(0.3)
    g_table = jnp.zeros((2 * heads, size), F32)
    steps = count // unroll
    parts = 4
    for k in range(parts):
        g_table = lax.fori_loop(k * steps // parts, (k + 1) * steps // parts, collect, g_table)
        if remote:
            run_due(2.2 / parts)
    g_table = g_table[:heads] + g_table[heads:]
    if not remote:
        r["out_table"][...] = g_table[:, :entries]
        return
    refs = [r[f"t_{k}"] for k in ("t0", "r0", "t1", "r1", "r2", "t3")]
    for k in range(2):
        refs[0][k] = g_table[k * heads // 2 : (k + 1) * heads // 2]

    def table_done(value):
        for k in range(2):
            r["out_table"][k * heads // 2 : (k + 1) * heads // 2, :] = value[k, :, :entries]

    n = pairs + 2 + groups
    last = Table(place, refs, r["send"].at[n], r["recv"].at[n], clock, table_done)
    last.start()
    active.append(last)
    run_due(0.0, True)


def local_grads(remote, tokens, cotangent, regions, rel_index, w_qkv, w_proj, bias_table):
    win, count, dim = tokens.shape
    entries, heads = bias_table.shape
    groups = heads // GROUP
    rows = win * PAD
    wide = GROUP * (dim // heads)
    size = -(-entries // 128) * 128
    own = dim // 32
    inputs = dict(
        reg=regions,
        rel=rel_index,
        table=bias_table.T,
        tok=tokens.transpose(1, 0, 2),
        w_qkv=w_qkv,
        cot=cotangent.transpose(1, 0, 2),
        w_proj=w_proj,
    )
    if remote:
        outs = dict(
            out_qkv=(own * 3 * dim // 128, 128), out_proj=(own * dim // 128, 128), out_table=(heads, entries)
        )
    else:
        outs = dict(out_qkv=(dim, 3 * dim), out_proj=(dim, dim), out_table=(heads, entries))
    vmem = pltpu.VMEM
    scratch = {f"{n}_vm": vmem(v.shape, v.dtype) for n, v in inputs.items()}
    scratch |= dict(
        fetch=pltpu.SemaphoreType.DMA((len(inputs),)),
        flat=vmem((dim // 128, rows, 128), F32),
        x=vmem((rows, dim), BF16),
        xt=vmem((dim, rows), BF16),
        c=vmem((rows, dim), BF16),
        qkv=vmem((rows, 3 * dim), BF16),
        d_att=vmem((rows, dim), BF16),
        att_t=vmem((dim, rows), BF16),
        d_v=vmem((rows, dim), BF16),
        d_qk=vmem((2, rows, 2 * wide), BF16),
        ring=vmem((2 * BATCH, PAD, GROUP * PAD), F32),
        ring_ds=vmem((2 * BATCH, PAD, GROUP * PAD), BF16),
        probs=vmem((groups, rows, GROUP * PAD), BF16),
        masks=vmem((rows, 128), F32),
        bias=vmem((groups, PAD, GROUP * PAD), F32),
        bias_rows=vmem((PAD * heads, 128), F32),
        d_bias=vmem((groups, PAD, GROUP * PAD), F32),
        small=vmem((128, 128), F32),
        rel_t=vmem((128, 128), F32),
        tab=vmem((heads, size), F32),
    )
    params = dict()
    if remote:
        chunks = {f"v{n}": 2 * wide for n in range(groups // 2)} | dict(p0=dim // 2, p1=dim // 2)
        chunks |= {f"k{g}": 2 * wide for g in range(groups)}
        for name, cols in chunks.items():
            if name[0] == "v":
                scratch[f"{name}_buf"] = vmem((2, 4, 2, 2, 2, 8, cols), F32)
                scratch[f"{name}_r0"] = vmem((4, 2, 2, 2, 8, cols), F32)
                scratch[f"{name}_r1"] = vmem((3, 2, 2, 2, 8, cols), F32)
                scratch[f"{name}_r2"] = vmem((2, 2, 8, cols), F32)
                scratch[f"{name}_s2"] = vmem((2, 2, 2, 8, cols), F32)
                scratch[f"{name}_r3"] = vmem((2, 8, cols), F32)
                continue
            scratch[f"{name}_buf"] = vmem((2, 2, 2, 2, 4, 8, cols), F32)
            scratch[f"{name}_r0"] = vmem((2, 2, 2, 4, 8, cols), F32)
            scratch[f"{name}_r1"] = vmem((2, 2, 4, 8, cols), F32)
            scratch[f"{name}_r2"] = vmem((2, 4, 8, cols), F32)
            scratch[f"{name}_s2"] = vmem((4, 2, 8, cols), F32)
            scratch[f"{name}_r3"] = vmem((3, 2, 8, cols), F32)
        for name, lead in dict(t0=(2,), r0=(), t1=(), r1=(3,), r2=(4,), t3=(2,)).items():
            scratch[f"t_{name}"] = vmem((*lead, heads // 2, size), F32)
        scratch["send"] = pltpu.SemaphoreType.DMA((len(chunks) + 1, COPIES))
        scratch["recv"] = pltpu.SemaphoreType.DMA((len(chunks) + 1, COPIES))
        params = dict(collective_id=0, has_side_effects=True)
    dims = (win, count, dim, heads, entries, remote)
    spec = pl.BlockSpec(memory_space=pltpu.VMEM)
    return pl.pallas_call(
        functools.partial(kernel, dims, [*inputs, *outs, *scratch]),
        out_shape=[jax.ShapeDtypeStruct(o, F32) for o in outs.values()],
        in_specs=[pl.BlockSpec(memory_space=pl.ANY)] * len(inputs),
        out_specs=[spec] * len(outs),
        scratch_shapes=list(scratch.values()),
        compiler_params=pltpu.CompilerParams(vmem_limit_bytes=60 * 1024 * 1024, **params),
    )(*inputs.values())


def momentum_kernel(norm, *refs):
    for grad, old, new in zip(refs[:3], refs[3:6], refs[6:], strict=True):
        new[...] = 0.9 * old[...] + grad[...] * norm


def momentum(norm, grads, moms):
    old = [m.reshape(g.shape) if m.ndim == 1 else m.T for g, m in zip(grads, moms, strict=True)]
    spec = pl.BlockSpec(memory_space=pltpu.VMEM)
    return pl.pallas_call(
        functools.partial(momentum_kernel, norm),
        out_shape=[jax.ShapeDtypeStruct(g.shape, F32) for g in grads],
        in_specs=[spec] * 6,
        out_specs=[spec] * 3,
    )(*grads, *old)


def body(
    tokens, cotangent, regions, rel_index, w_qkv, w_proj, bias_table, mom_qkv, mom_proj, mom_table
):
    dim = tokens.shape[2]
    devices = lax.axis_size(AXES)
    sizes = tuple(lax.axis_size(a) for a in AXES)
    norm = 1.0 / (tokens.shape[0] * devices)
    args = (tokens, cotangent, regions, rel_index, w_qkv, w_proj, bias_table)
    if sizes == (2, 4, 4) and dim == 16 * devices:
        grads = local_grads(True, *args)
        qkv, proj, table = momentum(norm, grads, (mom_qkv, mom_proj, mom_table))
        return qkv.reshape(-1), proj.reshape(-1), table.T
    qkv, proj, table = local_grads(False, *args)
    qkv_mine = lax.psum_scatter(qkv.reshape(-1), AXES, tiled=True)
    proj_mine = lax.psum_scatter(proj.reshape(-1), AXES, tiled=True)
    table = lax.psum(table, AXES)
    return (
        0.9 * mom_qkv + qkv_mine * norm,
        0.9 * mom_proj + proj_mine * norm,
        0.9 * mom_table + table.T * norm,
    )


def solution(mesh):
    return jax.shard_map(
        body,
        mesh=mesh,
        in_specs=(
            P(AXES, None, None),
            P(AXES, None, None),
            P(AXES, None),
            P(),
            P(),
            P(),
            P(),
            P(AXES),
            P(AXES),
            P(),
        ),
        out_specs=(P(AXES), P(AXES), P()),
        check_vma=False,
    )
```
